32 devices in a mesh: groups: 2 (over y), rows: 4 (over z), cols: 4 (over x, core), depth: 1.
Axes of the slice: x: 2, y: 2, z: 4, core: 2. Of those that a mesh axis runs over, the one named last changes fastest.
Arguments:
- tensor: float32 [128, 64, 128], P(('groups', 'rows'), 'cols', 'depth'), parts along dimension 0, may hold values from -6 to 6
- start_one: float32 [128, 64], P(('groups', 'rows')), parts along dimension 0, may hold values from -0.75 to 0.75
- start_two: float32 [128, 64], P(('groups', 'cols')), parts along dimension 0, may hold values from -0.75 to 0.75
- start_three: float32 [256, 32], P(('groups', 'depth')), parts along dimension 0, may hold values from -0.5 to 0.5
Outputs:
- final_one: float32 [128, 64], P(('groups', 'rows')), parts along dimension 0
- final_two: float32 [128, 64], P(('groups', 'cols')), parts along dimension 0
- final_three: float32 [256, 32], P(('groups', 'depth')), parts along dimension 0
- core_tensor: float32 [128, 64, 32], P('groups'), parts along dimension 0
The draws below stay inside these ranges and needn't reach their ends.
There are 2 independent parts, one for each index of `groups`. The reference program is written for one: setup_inputs(seed, part) draws one part's arguments, and reference() takes and returns one part's arrays. A program takes and returns all parts, laid end to end along the dimension named above; each array names one. Nothing has to cross between parts.
All inputs are finite; a program needn't handle non-finite values.
Results may differ from the reference program's by a relative error of at most 0.0001.
Values sent between devices are 32-bit elements; how exact they have to be, the bound alone decides.
A program may use at most 64 MiB of HBM per device.

```python
import math
import jax
import jax.numpy as jnp
from jax import lax

RANK_ONE = 64
RANK_TWO = 64
RANK_THREE = 32
SWEEPS = 1
NEWTON = 3
DIM_ONE = 64
DIM_TWO = 64
DIM_THREE = 128


def shard_levels(stream_key, shape, shards, low, high):
    def one(dim, shards_of):
        heights = jax.random.uniform(jax.random.fold_in(jax.random.fold_in(stream_key, 6), dim), (shards_of,), jnp.float32, low / len(shards), high / len(shards))
        return jnp.repeat(jnp.exp(heights), shape[dim] // shards_of).reshape((-1,) + (1,) * (len(shape) - dim - 1))

    gain = one(*shards[0])
    for cut in shards[1:]:
        gain = gain * one(*cut)
    return gain


def noise(key, shape, scale, most, pieces=(), kind=jnp.bfloat16):
    result = scale * jax.random.normal(key, shape, jnp.float32)
    if pieces:
        result = result * shard_levels(key, shape, pieces, -0.22, 0.18)
    return jnp.clip(result, -most, most).astype(kind)


def setup_inputs(seed: int = 0, part: int = 0) -> dict:
    keys = jax.random.split(jax.random.key(seed), 5)
    part_splits = jax.random.split(jax.random.fold_in(keys[4], part), 5)
    tensor = noise(part_splits[0], (DIM_ONE, DIM_TWO, DIM_THREE), 1.0, 6.0, ((0, 4), (1, 4)), jnp.float32)
    start_one = noise(part_splits[1], (DIM_ONE, RANK_ONE), DIM_ONE ** -0.5, 0.75, ((0, 4),), jnp.float32)
    start_two = noise(part_splits[2], (DIM_TWO, RANK_TWO), DIM_TWO ** -0.5, 0.75, ((0, 4),), jnp.float32)
    start_three = noise(part_splits[3], (DIM_THREE, RANK_THREE), DIM_THREE ** -0.5, 0.5, (), jnp.float32)
    return dict(tensor=tensor, start_one=start_one, start_two=start_two, start_three=start_three)


exact_mode = lax.Precision.HIGHEST

def newton_steps(matrix):
    gram_matrix = jnp.dot(matrix.T, matrix, precision=exact_mode)
    total = jnp.trace(gram_matrix) + 1e-06
    current = matrix / jnp.sqrt(total)
    gram_matrix = gram_matrix / total
    identity = jnp.eye(matrix.shape[1], dtype=jnp.float32)
    for newton_index in range(NEWTON):
        if newton_index > 0:
            gram_matrix = jnp.dot(current.T, current, precision=exact_mode)
        current = jnp.dot(current, 1.5 * identity - 0.5 * gram_matrix, precision=exact_mode)
    return current

def reference(tensor, start_one, start_two, start_three):
    first, second, third = (start_one, start_two, start_three)
    core_flat = None
    for sweep_index in range(SWEEPS):
        sectioned = jnp.einsum('ijk,jb->bik', tensor, second, precision=exact_mode)
        unfolded = jnp.einsum('bik,kc->ibc', sectioned, third, precision=exact_mode).reshape(DIM_ONE, RANK_TWO * RANK_THREE)
        core_flat = jnp.dot(first.T, unfolded, precision=exact_mode)
        first = newton_steps(jnp.dot(unfolded, core_flat.T, precision=exact_mode))
        sectioned = jnp.einsum('ijk,ia->ajk', tensor, first, precision=exact_mode)
        unfolded = jnp.einsum('ajk,kc->jac', sectioned, third, precision=exact_mode).reshape(DIM_TWO, RANK_ONE * RANK_THREE)
        core_flat = jnp.dot(second.T, unfolded, precision=exact_mode)
        second = newton_steps(jnp.dot(unfolded, core_flat.T, precision=exact_mode))
        unfolded = jnp.einsum('ajk,jb->kab', sectioned, second, precision=exact_mode).reshape(DIM_THREE, RANK_ONE * RANK_TWO)
        core_flat = jnp.dot(third.T, unfolded, precision=exact_mode)
        third = newton_steps(jnp.dot(unfolded, core_flat.T, precision=exact_mode))
    core_tensor = core_flat.reshape(RANK_THREE, RANK_ONE, RANK_TWO).transpose(1, 2, 0)
    return (first * math.sqrt(DIM_ONE), second * math.sqrt(DIM_TWO), third * math.sqrt(DIM_THREE), core_tensor)
```

```python
import functools
import math

import jax
import jax.numpy as jnp
from jax import lax
from jax.experimental import pallas as pl
from jax.experimental.pallas import tpu as pltpu
from jax.sharding import PartitionSpec as P

NEWTON = 3


exact_mode = lax.Precision.HIGHEST


def newton_steps(matrix, reduce_gram):
    gram_matrix = reduce_gram(jnp.dot(matrix.T, matrix, precision=exact_mode))
    total = jnp.trace(gram_matrix) + 1e-06
    current = matrix / jnp.sqrt(total)
    gram_matrix = gram_matrix / total
    identity = jnp.eye(matrix.shape[1], dtype=jnp.float32)
    for newton_index in range(NEWTON):
        if newton_index > 0:
            gram_matrix = reduce_gram(jnp.dot(current.T, current, precision=exact_mode))
        current = jnp.dot(current, 1.5 * identity - 0.5 * gram_matrix, precision=exact_mode)
    return current


def general_body(tensor, start_one, start_two, start_three):
    first, second, third = (start_one, start_two, start_three)
    block_one, block_two, block_three = tensor.shape
    rank_one = first.shape[1]
    rank_two = second.shape[1]
    rank_three = third.shape[1]
    core_flat = None
    sectioned = jnp.einsum("ijk,jb->bik", tensor, second, precision=exact_mode)
    unfolded = jnp.einsum("bik,kc->ibc", sectioned, third, precision=exact_mode).reshape(
        block_one, rank_two * rank_three
    )
    share = lax.psum_scatter(unfolded, ("cols", "depth"), scatter_dimension=1, tiled=True)
    piece = lax.psum(jnp.dot(first.T, share, precision=exact_mode), "rows")
    z_part = jnp.dot(share, piece.T, precision=exact_mode)
    z_rows = lax.psum(z_part, ("cols", "depth"))
    first = newton_steps(z_rows, lambda matrix: lax.psum(matrix, "rows"))
    sectioned = jnp.einsum("ijk,ia->ajk", tensor, first, precision=exact_mode)
    unfolded = jnp.einsum("ajk,kc->jac", sectioned, third, precision=exact_mode).reshape(
        block_two, rank_one * rank_three
    )
    share = lax.psum_scatter(unfolded, ("rows", "depth"), scatter_dimension=1, tiled=True)
    piece = lax.psum(jnp.dot(second.T, share, precision=exact_mode), "cols")
    z_part = jnp.dot(share, piece.T, precision=exact_mode)
    z_rows = lax.psum(z_part, ("rows", "depth"))
    second = newton_steps(z_rows, lambda matrix: lax.psum(matrix, "cols"))
    unfolded = jnp.einsum("ajk,jb->kab", sectioned, second, precision=exact_mode).reshape(
        block_three, rank_one * rank_two
    )
    core_flat = lax.psum(
        jnp.dot(third.T, unfolded, precision=exact_mode), ("rows", "cols", "depth")
    )
    z_rows = lax.psum(jnp.dot(unfolded, core_flat.T, precision=exact_mode), ("rows", "cols"))
    third = newton_steps(z_rows, lambda matrix: lax.psum(matrix, "depth"))
    core_tensor = core_flat.reshape(rank_three, rank_one, rank_two).transpose(1, 2, 0)
    length_one = block_one * lax.axis_size("rows")
    length_two = block_two * lax.axis_size("cols")
    length_three = block_three * lax.axis_size("depth")
    return (
        first * math.sqrt(length_one),
        second * math.sqrt(length_two),
        third * math.sqrt(length_three),
        core_tensor,
    )


LANES = 128
SUBLANES = 8
VMEM_GRANT = 24 * 1024 * 1024
MESH = pl.DeviceIdType.MESH


def split(x):
    high = x.astype(jnp.bfloat16)
    low = (x - high.astype(jnp.float32)).astype(jnp.bfloat16)
    return high, low


def raw(a, b, dims=((1,), (0,))):
    return lax.dot_general(a, b, (dims, ((), ())), preferred_element_type=jnp.float32)


def mm(a, b, dims=((1,), (0,))):
    ah, al = split(a)
    bh, bl = split(b)
    return raw(ah, bh, dims) + (raw(al, bh, dims) + raw(ah, bl, dims))


def eye(n):
    return (lax.broadcasted_iota(jnp.int32, (n, n), 0) == lax.broadcasted_iota(jnp.int32, (n, n), 1)).astype(jnp.float32)


def products(lefts, b):
    parts = [split(a) for a in lefts]
    bh, bl = split(b)
    top = raw(jnp.concatenate([p[0] for p in parts] + [p[1] for p in parts], axis=0), bh)
    bottom = raw(jnp.concatenate([p[0] for p in parts], axis=0), bl)
    half, results, at = bottom.shape[0], [], 0
    for a in lefts:
        n = a.shape[0]
        results.append(top[at:at + n] + (top[half + at:half + at + n] + bottom[at:at + n]))
        at += n
    return results


def normalized(z, gram):
    total = jnp.sum(z * z, axis=(0, 1), keepdims=True) + 1e-06
    return gram * (1.0 / total), 1.0 / jnp.sqrt(total)


def next_gram(gram, square):
    return mm(gram, 2.25 * eye(gram.shape[0]) - 1.5 * gram + 0.25 * square)


def orth(z, carried=None):
    gram, scale = normalized(z, mm(z, z, ((0,), (0,))))
    for n in range(NEWTON - 1):
        step, square = products([z, gram], gram)
        z = 1.5 * z - 0.5 * step
        gram = next_gram(gram, square)
    result = (1.5 * z - 0.5 * mm(z, gram)) * scale
    if carried is None:
        return result
    inner = mm(z, carried, ((0,), (0,)))
    return result, (1.5 * inner - 0.5 * mm(gram, inner)) * scale


def orth_rows(z):
    gram, scale = normalized(z, mm(z, z, ((1,), (1,))))
    for n in range(NEWTON - 1):
        square = mm(gram, gram)
        z = 1.5 * z - 0.5 * mm(gram, z)
        gram = next_gram(gram, square)
    return (1.5 * z - 0.5 * mm(gram, z)) * scale


def turn(x, width):
    row = lax.broadcasted_iota(jnp.int32, x.shape, 1)
    group = lax.broadcasted_iota(jnp.int32, x.shape, 2) // width
    result = x
    for d in range(1, SUBLANES):
        moved = pltpu.roll(pltpu.roll(x, SUBLANES - d, 1), d * width, 2)
        result = jnp.where((group - row + SUBLANES) % SUBLANES == d, moved, result)
    return result


def pair_gram(cat):
    n = cat.shape[0]
    high, low = split(cat)
    both = jnp.concatenate([high, low], axis=0)
    prod = raw(both, both, ((1,), (1,)))
    return prod[:n, :n] + (prod[n:, :n] + prod[:n, n:])


def kernel(n_r, n_c, t_hbm, u1_hbm, u2_hbm, u3_hbm, o1_ref, o2_ref, zsum_ref, core_ref,
           t_ref, u1_ref, u2_ref, u3_ref, load_sem, mine, abuf, u1buf, u2buf, kron, at, work, tbuf, zrow,
           a_send, a_recv, f_send, f_recv, u1_send, u1_recv, u2_send, u2_recv,
           t_send, t_recv, tf_send, tf_recv, zr_send, zr_recv):
    g = lax.axis_index("groups")
    r = lax.axis_index("rows")
    cl = lax.axis_index("cols")
    bi, bj, bk = t_ref.shape
    r1, r2, r3 = u1_ref.shape[1], u2_ref.shape[1], u3_ref.shape[0]
    lo = LANES // bj
    hi = r3 // lo
    n_x = n_c // 2
    d1, d2 = n_r * bi, n_c * bj
    ihi = bi // SUBLANES

    def device(rr, cc):
        return (g, rr, cc, 0)

    def col(dx, parity):
        return lax.rem(cl // 2 + dx, n_x) * 2 + parity

    def row(dr):
        return lax.rem(r + dr, n_r)

    def far_row(n):
        up = r // (n_r // 2)
        here = r + up * (n_r - 1 - 2 * r)
        there = n_r - 1 - n - (here + n + 1) // n_r
        return there + up * (n_r - 1 - 2 * there)

    own, other = lax.rem(cl, 2), 1 - lax.rem(cl, 2)

    loads = [
        pltpu.make_async_copy(src, dst, load_sem.at[n])
        for n, (src, dst) in enumerate((
            (t_hbm, t_ref), (u3_hbm, u3_ref), (u2_hbm, u2_ref), (u1_hbm, u1_ref),
            (u2_hbm, u2buf.at[cl]), (u1_hbm, u1buf.at[r]), (t_hbm, tbuf.at[cl])))
    ]
    for load in loads:
        load.start()

    barrier = pltpu.get_barrier_semaphore()
    for dr in range(n_r):
        for dc in range(n_c):
            if dr or dc:
                pl.semaphore_signal(barrier, inc=1, device_id=device(row(dr), lax.rem(cl + dc, n_c)), device_id_type=MESH)

    for load in loads[:2]:
        load.wait()
    t2 = t_ref[...].reshape(bi * bj, bk)
    x = mm(u3_ref[...], t2, ((1,), (1,)))
    tiles = jnp.stack([x[h * lo:(h + 1) * lo, q * LANES:(q + 1) * LANES] for h in range(hi) for q in range(ihi)])
    turned = turn(tiles, bj).reshape(hi, bi, LANES)
    mine[...] = turned
    abuf[cl, :, pl.ds(pl.multiple_of(r * bi, bi), bi), :] = turned

    for load in loads[2:]:
        load.wait()
    pl.semaphore_wait(barrier, n_r * n_c - 1)

    def slot(rr, cc):
        return abuf.at[cc, :, pl.ds(pl.multiple_of(rr * bi, bi), bi), :]

    sends = []

    def push(src, dst, s_sem, r_sem, dev):
        copy = pltpu.make_async_remote_copy(src_ref=src, dst_ref=dst, send_sem=s_sem, recv_sem=r_sem, device_id=dev, device_id_type=MESH)
        copy.start()
        sends.append(copy)

    def await_in(dst, s_sem, r_sem, dev):
        pltpu.make_async_remote_copy(src_ref=dst, dst_ref=dst, send_sem=s_sem, recv_sem=r_sem, device_id=dev, device_id_type=MESH).wait_recv()

    for dc in range(1, n_c):
        push(u2_ref, u2buf.at[cl], u2_send.at[dc], u2_recv.at[dc], device(r, lax.rem(cl + dc, n_c)))
    order = [(dr, dx) for dr in range(n_r) for dx in range(n_x) if dr or dx]
    for dr, dx in order:
        n = dr * n_x + dx
        push(mine, slot(r, cl), a_send.at[n], a_recv.at[n], device(row(dr), col(dx, own)))
    push(mine, slot(r, cl), f_send.at[0], f_recv.at[0], device(r, col(0, other)))
    for dr in range(1, n_r):
        push(u1_ref, u1buf.at[r], u1_send.at[dr], u1_recv.at[dr], device(row(dr), cl))

    for dx in range(1, n_x):
        push(t_ref, tbuf.at[cl], t_send.at[dx], t_recv.at[dx], device(r, col(dx, own)))
    push(t_ref, tbuf.at[cl], tf_send.at[0], tf_recv.at[0], device(r, col(0, other)))

    for dc in range(1, n_c):
        src = lax.rem(cl + n_c - dc, n_c)
        await_in(u2buf.at[src], u2_send.at[dc], u2_recv.at[dc], device(r, src))
    mask = (lax.broadcasted_iota(jnp.int32, (LANES, lo * r2), 0) // bj) == (lax.broadcasted_iota(jnp.int32, (LANES, lo * r2), 1) // r2)
    for c in range(n_c):
        block = jnp.concatenate([u2buf[c]] * lo, axis=0)
        block = jnp.concatenate([block, block], axis=1)
        block = jnp.where(mask, jnp.concatenate([block] * (lo // 2), axis=1), 0.0)
        kh, kl = split(block)
        kron[0, c * LANES:(c + 1) * LANES, :] = kh
        kron[1, c * LANES:(c + 1) * LANES, :] = kl

    for dr, dx in order:
        n = dr * n_x + dx
        rr, cc = lax.rem(r + n_r - dr, n_r), lax.rem(cl // 2 + n_x - dx, n_x) * 2 + own
        await_in(slot(rr, cc), a_send.at[n], a_recv.at[n], device(rr, cc))
        push(slot(rr, cc), slot(rr, cc), f_send.at[n], f_recv.at[n], device(r, col(0, other)))
    for dr, dx in [(0, 0)] + order:
        n = dr * n_x + dx
        rr, cc = lax.rem(r + n_r - dr, n_r), lax.rem(cl // 2 + n_x - dx, n_x) * 2 + other
        await_in(slot(rr, cc), f_send.at[n], f_recv.at[n], device(r, col(0, other)))
    for dr in range(1, n_r):
        src = lax.rem(r + n_r - dr, n_r)
        await_in(u1buf.at[src], u1_send.at[dr], u1_recv.at[dr], device(src, cl))

    block = jnp.concatenate([abuf[c].reshape(hi * d1, LANES) for c in range(n_c)], axis=1)
    bh, bl = split(block)
    kh = kron[0]
    y1 = raw(bh, kh) + (raw(bl, kh) + raw(bh, kron[1]))
    m1 = pair_gram(jnp.concatenate([y1[h * d1:(h + 1) * d1] for h in range(hi)], axis=1))
    bhf, blf = bh.astype(jnp.float32), bl.astype(jnp.float32)
    for h in range(hi):
        part = jnp.concatenate([bhf[h * d1:(h + 1) * d1], blf[h * d1:(h + 1) * d1]], axis=0)
        at[h] = part.T.astype(jnp.bfloat16)
    for dx in range(1, n_x):
        cc = lax.rem(cl // 2 + n_x - dx, n_x) * 2 + own
        await_in(tbuf.at[cc], t_send.at[dx], t_recv.at[dx], device(r, cc))
        push(tbuf.at[cc], tbuf.at[cc], tf_send.at[dx], tf_recv.at[dx], device(r, col(0, other)))

    first = orth(mm(m1, u1buf[...].reshape(d1, r1)))
    work[0] = first
    first_own = work[0, pl.ds(pl.multiple_of(r * bi, bi), bi), :]
    o1_ref[...] = first_own * math.sqrt(d1)

    fh, fl = split(first)
    zero = jnp.zeros_like(fh)
    rhs = jnp.concatenate([
        jnp.concatenate([fh, zero, fl, zero], axis=1),
        jnp.concatenate([fh, zero, zero, zero], axis=1),
        jnp.concatenate([zero, fh, zero, fl], axis=1),
        jnp.concatenate([zero, fh, zero, zero], axis=1)], axis=0)
    pieces = []
    for h in range(hi):
        even = jnp.concatenate([at[h, (q * lo + s) * bj:(q * lo + s + 1) * bj, :] for s in range(0, lo, 2) for q in range(n_c)], axis=0)
        odd = jnp.concatenate([at[h, (q * lo + s) * bj:(q * lo + s + 1) * bj, :] for s in range(1, lo, 2) for q in range(n_c)], axis=0)
        prod = raw(jnp.concatenate([even, odd], axis=1), rhs)
        prod = prod[:, :2 * r1] + prod[:, 2 * r1:]
        pieces += [prod[s * d2:(s + 1) * d2] for s in range(lo // 2)]
    y2 = jnp.concatenate(pieces, axis=1)
    m2 = pair_gram(y2)
    spread = jnp.concatenate([first_own] * lo, axis=0)
    spread = jnp.concatenate([spread, spread], axis=1)
    spread = jnp.concatenate([spread] * (lo // 2), axis=1)
    mask3 = (lax.broadcasted_iota(jnp.int32, (LANES, lo * r1), 0) // bi) == (lax.broadcasted_iota(jnp.int32, (LANES, lo * r1), 1) // r1)
    spread = jnp.where(mask3, spread, 0.0)
    wide = jnp.concatenate([y2[:, h * lo * r1:(h + 1) * lo * r1] for h in range(hi)], axis=0)
    wide = mm(wide, spread, ((1,), (1,)))
    wide = jnp.concatenate([wide[h * d2:(h + 1) * d2] for h in range(hi)], axis=1)
    for dx in range(n_x):
        cc = lax.rem(cl // 2 + n_x - dx, n_x) * 2 + other
        await_in(tbuf.at[cc], tf_send.at[dx], tf_recv.at[dx], device(r, col(0, other)))
    tperm = jnp.concatenate([tbuf[c, :, j, :] for c in range(n_c) for j in range(bj)], axis=0)
    th, tl = split(tperm)
    second, inner = orth(mm(m2, u2buf[...].reshape(d2, r2)), wide)
    work[1] = second
    second_own = work[1, pl.ds(pl.multiple_of(cl * bj, bj), bj), :]
    o2_ref[...] = second_own * math.sqrt(d2)

    w = mm(second, inner)
    jhi = d2 // SUBLANES
    w = jnp.concatenate([w[:, h * LANES:(h + 1) * LANES] for h in range(hi)], axis=0)
    w = turn(w.reshape(hi * jhi, SUBLANES, LANES), bi)
    w = jnp.concatenate([jnp.concatenate([w[h * jhi + q] for q in range(jhi)], axis=1) for h in range(hi)], axis=0)
    wh, wl = split(w)
    z = raw(jnp.concatenate([wh, wl], axis=0), th)
    z = z[:r3] + (z[r3:] + raw(wh, tl))
    zrow[r] = z
    for n in range(n_r - 1):
        push(zrow.at[r], zrow.at[r], zr_send.at[n], zr_recv.at[r], device(far_row(n), cl))

    yh, yl = split(y2)
    both = jnp.concatenate([yh.astype(jnp.float32), yl.astype(jnp.float32)], axis=0)
    sh, sl = split(second)
    high = jnp.concatenate([sh, sh], axis=0)
    low = jnp.concatenate([sl, jnp.zeros_like(sl)], axis=0)
    lhs = both.T.astype(jnp.bfloat16)
    core = (raw(lhs, high) + raw(lhs, low)).reshape(r3, r1, r2)

    for c in range(r3):
        core_ref[:, c, :] = core[c]
    for n in reversed(range(n_r - 1)):
        src = far_row(n)
        await_in(zrow.at[src], zr_send.at[n], zr_recv.at[src], device(src, cl))
    zsum_ref[...] = sum(zrow[n] for n in range(1, n_r)) + zrow[0]
    for copy in sends:
        copy.wait_send()


def finish(o1_ref, o2_ref, zsum_ref, core_ref, o1_hbm, o2_hbm, o3_hbm, core_hbm, o3_ref, sem):
    def out(n, src, dst):
        copy = pltpu.make_async_copy(src, dst, sem.at[n])
        copy.start()
        return copy

    copies = [out(0, core_ref, core_hbm), out(1, o1_ref, o1_hbm), out(2, o2_ref, o2_hbm)]
    o3_ref[...] = orth_rows(zsum_ref[...]) * math.sqrt(zsum_ref.shape[1])
    copies.append(out(3, o3_ref, o3_hbm))
    for copy in copies:
        copy.wait()


def fused_body(tensor, start_one, start_two, start_three):
    n_r, n_c = lax.axis_size("rows"), lax.axis_size("cols")
    bi, bj, bk = tensor.shape
    r1, r2, r3 = start_one.shape[1], start_two.shape[1], start_three.shape[1]
    lo = LANES // bj
    hi = r3 // lo
    d1, d2 = n_r * bi, n_c * bj
    f32, bf16 = jnp.float32, jnp.bfloat16
    vmem = pl.BlockSpec(memory_space=pltpu.VMEM)
    anywhere = pl.BlockSpec(memory_space=pl.ANY)
    dma = pltpu.SemaphoreType.DMA
    n_a = n_r * n_c // 2
    final_one, final_two, final_three, core = pl.pallas_call(
        functools.partial(kernel, n_r, n_c),
        out_shape=(
            jax.ShapeDtypeStruct((bi, r1), f32),
            jax.ShapeDtypeStruct((bj, r2), f32),
            jax.ShapeDtypeStruct((r3, bk), f32),
            jax.ShapeDtypeStruct((r1, r3, r2), f32),
        ),
        in_specs=[pl.BlockSpec(memory_space=pltpu.HBM)] * 4,
        out_specs=[vmem] * 4,
        scratch_shapes=[
            pltpu.VMEM((bi, bj, bk), f32),
            pltpu.VMEM((bi, r1), f32),
            pltpu.VMEM((bj, r2), f32),
            pltpu.VMEM((r3, bk), f32),
            dma((7,)),
            pltpu.VMEM((hi, bi, LANES), f32),
            pltpu.VMEM((n_c, hi, d1, LANES), f32),
            pltpu.VMEM((n_r, bi, r1), f32),
            pltpu.VMEM((n_c, bj, r2), f32),
            pltpu.VMEM((2, n_c * LANES, lo * r2), bf16),
            pltpu.VMEM((hi, n_c * LANES, 2 * d1), bf16),
            pltpu.VMEM((2, max(d1, d2), max(r1, r2)), f32),
            pltpu.VMEM((n_c, bi, bj, bk), f32),
            pltpu.VMEM((n_r, r3, bk), f32),
            dma((n_a,)), dma((n_a,)), dma((n_a,)), dma((n_a,)),
            dma((n_r,)), dma((n_r,)), dma((n_c,)), dma((n_c,)),
            dma((n_c // 2,)), dma((n_c // 2,)), dma((n_c // 2,)), dma((n_c // 2,)),
            dma((n_r,)), dma((n_r,)),
        ],
        compiler_params=pltpu.CompilerParams(collective_id=0, has_side_effects=True, vmem_limit_bytes=VMEM_GRANT),
    )(*(pltpu.with_memory_space_constraint(x, pltpu.HBM) for x in (tensor, start_one, start_two, start_three.T)))
    results = (final_one, final_two, final_three, core)
    final_one, final_two, final_three, core = pl.pallas_call(
        finish,
        out_shape=tuple(jax.ShapeDtypeStruct(x.shape, f32) for x in results),
        in_specs=[vmem] * 4,
        out_specs=[anywhere] * 4,
        scratch_shapes=[pltpu.VMEM((r3, bk), f32), dma((4,))],
        compiler_params=pltpu.CompilerParams(vmem_limit_bytes=VMEM_GRANT),
    )(*results)
    return final_one, final_two, final_three.T, core.transpose(0, 2, 1)


def body(tensor, start_one, start_two, start_three):
    bi, bj, bk = tensor.shape
    r1, r2, r3 = start_one.shape[1], start_two.shape[1], start_three.shape[1]
    n_r, n_c = lax.axis_size("rows"), lax.axis_size("cols")
    fits = (
        lax.axis_size("depth") == 1
        and n_c % 2 == 0
        and bi * SUBLANES == LANES
        and bj * SUBLANES == LANES
        and r3 % SUBLANES == 0
        and 2 * r1 == LANES
        and 2 * r2 == LANES
        and 2 * n_r * bi == LANES
        and 2 * n_c * bj == LANES
        and bk % LANES == 0
    )
    return (fused_body if fits else general_body)(tensor, start_one, start_two, start_three)


def solution(mesh):
    in_specs = (
        P(("groups", "rows"), "cols", "depth"),
        P(("groups", "rows"), None),
        P(("groups", "cols"), None),
        P(("groups", "depth"), None),
    )
    out_specs = (
        P(("groups", "rows"), None),
        P(("groups", "cols"), None),
        P(("groups", "depth"), None),
        P("groups", None, None),
    )
    return jax.shard_map(body, mesh=mesh, in_specs=in_specs, out_specs=out_specs, check_vma=False)
```
